256 devices in a mesh: tile: 64 (over z, y_hi, x), sub: 4 (over y_lo, core).
Axes of the slice: x: 4, y: 4 (y_hi: 2, y_lo: 2; y = y_hi * 2 + y_lo), z: 8, core: 2. Of those that a mesh axis runs over, the one named last changes fastest.
Arguments:
- grid_feats: bfloat16 [32768, 512], P(('tile', 'sub')), may hold values from -6 to 6
- mesh_feats: bfloat16 [32768, 512], P(('tile', 'sub')), may hold values from -6 to 6
- encode_edges: bfloat16 [262144, 512], P(('tile', 'sub')), may hold values from -6 to 6
- decode_edges: bfloat16 [131072, 512], P(('tile', 'sub')), may hold values from -6 to 6
- encode_source: int32 [262144], P(('tile', 'sub')), may hold values from 0 to 32767, as said below
- encode_target: int32 [262144], P(('tile', 'sub')), may hold values from -1 to 32767, as said below
- decode_source: int32 [131072], P(('tile', 'sub')), may hold values from 0 to 32767, as said below
- decode_target: int32 [131072], P(('tile', 'sub')), may hold values from -1 to 32767, as said below
- owner_fine: int32 [32768], P(('tile', 'sub')), may hold values from 0 to 8191, as said below
- owner_coarse: int32 [8192], P('tile'), may hold values from 0 to 511
- encode_weight: bfloat16 [512, 512], replicated, may hold values from -0.25 to 0.25
- decode_weight: bfloat16 [512, 512], replicated, may hold values from -0.25 to 0.25
- middle_weight: bfloat16 [512, 512], replicated, may hold values from -0.25 to 0.25
- summit_weight: bfloat16 [512, 512], replicated, may hold values from -0.25 to 0.25
- cotangent: bfloat16 [32768, 512], P(('tile', 'sub')), may hold values from -6 to 6
Outputs:
- grid_update: bfloat16 [32768, 512], P(('tile', 'sub'))
- encode_grad: float32 [512, 512], replicated
- decode_grad: float32 [512, 512], replicated
- middle_grad: float32 [512, 512], replicated
- summit_grad: float32 [512, 512], replicated
The draws below stay inside these ranges and needn't reach their ends.
Inputs may be any that keep to these rules, and one draw needn't show every extreme that they name: `encode_source`: edge slot e is listed on device d = e // 1024; its source grid node lies on device d - 1, d or d + 1. `encode_target`: -1 marks padding; every other value is a mesh node of the device that lists the slot. On each device padding fills whole blocks of 128 slots after all live ones; every device has a live block, and some device has no padding. `decode_source`: edge slot e is listed on device d = e // 512; its source mesh node lies on device d - 1, d or d + 1. `decode_target`: -1 marks padding; every other value is a grid node of the device that lists the slot. On each device padding fills whole blocks of 128 slots after all live ones; every device has a live block, and some device has no padding. `owner_fine`: the middle node of fine mesh node m lies on the tile of the device that holds m.
All inputs are finite; a program needn't handle non-finite values.
Results may differ from the reference program's by a relative error of at most 0.012.
Values may be sent and summed in bfloat16 or wider, within the bound.
A program may use at most 64 MiB of HBM per device.

```python
import jax
import jax.numpy as jnp

D = 512
GRID_DEV = 128
MESH_DEV = 128
MID_TILE = 128
TOP_NODES = 512
ENCODE_DEV = 1024
DECODE_DEV = 512
BLOCK = 128
GRID = 32768
MESH = 32768
MIDDLE = 8192
ENCODE = 262144
DECODE = 131072
N_TILE = 64
N_SUB = 4
DEVICES = 256


def near_senders(key, per_device, node_rows):
    device_of = jnp.arange(per_device * DEVICES, dtype=jnp.int32) // per_device
    lowest = jnp.maximum(device_of - 1, 0) * node_rows
    highest = jnp.minimum(device_of + 2, DEVICES) * node_rows
    return jax.random.randint(key, (per_device * DEVICES,), lowest, highest, dtype=jnp.int32)


def own_receivers(key, per_device, node_rows):
    blocks_each = per_device // BLOCK
    live_key = jax.random.fold_in(key, 11)
    full_key = jax.random.fold_in(key, 12)
    node_key = jax.random.fold_in(key, 13)
    live_blocks = jax.random.randint(live_key, (DEVICES,), 1, blocks_each + 1, dtype=jnp.int32)
    full_device = jax.random.randint(full_key, (), 0, DEVICES, dtype=jnp.int32)
    live_blocks = jnp.where(jnp.arange(DEVICES, dtype=jnp.int32) == full_device, blocks_each, live_blocks)
    edge_ids = jnp.arange(per_device * DEVICES, dtype=jnp.int32)
    device_of = edge_ids // per_device
    block_of = edge_ids % per_device // BLOCK
    chosen = jax.random.randint(node_key, (per_device * DEVICES,), device_of * node_rows, (device_of + 1) * node_rows, dtype=jnp.int32)
    return jnp.where(block_of < live_blocks[device_of], chosen, -1).astype(jnp.int32)


def draw_encode_source(key, part):
    return near_senders(jax.random.fold_in(key, 1), ENCODE_DEV, GRID_DEV)


def draw_encode_target(key, part):
    return own_receivers(jax.random.fold_in(key, 2), ENCODE_DEV, MESH_DEV)


def draw_decode_source(key, part):
    return near_senders(jax.random.fold_in(key, 3), DECODE_DEV, MESH_DEV)


def draw_decode_target(key, part):
    return own_receivers(jax.random.fold_in(key, 4), DECODE_DEV, GRID_DEV)


def draw_owner_fine(key, part):
    node_ids = jnp.arange(MESH_DEV * DEVICES, dtype=jnp.int32)
    tile_of = node_ids // MESH_DEV // N_SUB
    return jax.random.randint(jax.random.fold_in(key, 5), (MESH_DEV * DEVICES,), tile_of * MID_TILE, (tile_of + 1) * MID_TILE, dtype=jnp.int32)


def with_ends(drawn, rng, smallest, top_value):
    dims = drawn.shape
    spot = [jax.random.randint(jax.random.fold_in(rng, axis), (), 0, dims[axis]) for axis in range(len(dims))]
    drawn = drawn.at[tuple(spot)].set(smallest)
    longest = dims.index(max(dims))
    spot[longest] = (spot[longest] + 1) % dims[longest]
    return drawn.at[tuple(spot)].set(top_value)


def steps_of(key, extent, pieces, least, top_value):
    factor_of, own = 1.0, jax.random.fold_in(key, 6)
    for axis_at, blocks in pieces:
        draws = jnp.exp(jax.random.uniform(jax.random.fold_in(own, axis_at), (blocks,), jnp.float32, least / len(pieces), top_value / len(pieces)))
        factor_of = factor_of * jnp.repeat(draws, extent[axis_at] // blocks).reshape([-1 if axis == axis_at else 1 for axis in range(len(extent))])
    return factor_of


def noise(stream_key, extent, deviation, reach, pieces=(), kind=jnp.bfloat16):
    level = steps_of(stream_key, extent, pieces, -0.22, 0.18) if pieces else 1.0
    values = jax.random.normal(stream_key, extent, jnp.float32) * deviation * level
    return jnp.minimum(jnp.maximum(values, -reach), reach).astype(kind)


def setup_inputs(seed: int = 0) -> dict:
    key_of = jax.random.split(jax.random.key(seed), 16)
    grid_feats = noise(key_of[0], (GRID, D), 1.0, 6.0, ((0, 256),))
    mesh_feats = noise(key_of[1], (MESH, D), 1.0, 6.0, ((0, 256),))
    encode_edges = noise(key_of[2], (ENCODE, D), 1.0, 6.0, ((0, 256),))
    decode_edges = noise(key_of[3], (DECODE, D), 1.0, 6.0, ((0, 256),))
    encode_source = draw_encode_source(jax.random.fold_in(key_of[15], 71), 0)
    encode_target = draw_encode_target(jax.random.fold_in(key_of[15], 71), 0)
    decode_source = draw_decode_source(jax.random.fold_in(key_of[15], 71), 0)
    decode_target = draw_decode_target(jax.random.fold_in(key_of[15], 71), 0)
    owner_fine = draw_owner_fine(jax.random.fold_in(key_of[15], 71), 0)
    owner_coarse = with_ends(jax.random.randint(key_of[9], (MIDDLE,), 0, TOP_NODES), jax.random.fold_in(key_of[9], 1), 0, TOP_NODES - 1).astype(jnp.int32)
    encode_weight = noise(key_of[10], (D, D), D ** -0.5, 0.25)
    decode_weight = noise(key_of[11], (D, D), D ** -0.5, 0.25)
    middle_weight = noise(key_of[12], (D, D), D ** -0.5, 0.25)
    summit_weight = noise(key_of[13], (D, D), D ** -0.5, 0.25)
    cotangent = noise(key_of[14], (GRID, D), 1.0, 6.0, ((0, 256),))
    return dict(grid_feats=grid_feats, mesh_feats=mesh_feats, encode_edges=encode_edges, decode_edges=decode_edges, encode_source=encode_source, encode_target=encode_target, decode_source=decode_source, decode_target=decode_target, owner_fine=owner_fine, owner_coarse=owner_coarse, encode_weight=encode_weight, decode_weight=decode_weight, middle_weight=middle_weight, summit_weight=summit_weight, cotangent=cotangent)


def silu_slope(values):
    sigmoid = jax.nn.sigmoid(values)
    return sigmoid * (1.0 + values * (1.0 - sigmoid))


def edge_sum(values, targets, segments):
    aimed = jnp.where(targets >= 0, targets, segments).astype(jnp.int32)
    return jax.ops.segment_sum(values, aimed, num_segments=segments + 1)[:segments]


def reference(grid_feats, mesh_feats, encode_edges, decode_edges, encode_source, encode_target, decode_source, decode_target, owner_fine, owner_coarse, encode_weight, decode_weight, middle_weight, summit_weight, cotangent):
    encode_factor = MESH_DEV / ENCODE_DEV
    decode_factor = GRID_DEV / DECODE_DEV
    middle_factor = MID_TILE / (MESH_DEV * N_SUB)
    summit_factor = TOP_NODES / (MID_TILE * N_TILE)
    encode_rows = grid_feats[encode_source]
    encode_pre = jnp.dot(encode_rows, encode_weight, preferred_element_type=jnp.float32) + encode_edges.astype(jnp.float32)
    mesh_mid = (mesh_feats.astype(jnp.float32) + encode_factor * edge_sum(jax.nn.silu(encode_pre), encode_target, MESH)).astype(jnp.bfloat16)
    middle_sum = jax.ops.segment_sum(mesh_mid.astype(jnp.float32), owner_fine, num_segments=MIDDLE)
    middle_in = (middle_factor * middle_sum).astype(jnp.bfloat16)
    middle_act = jnp.dot(middle_in, middle_weight, preferred_element_type=jnp.float32)
    middle_out = (middle_in.astype(jnp.float32) + jax.nn.silu(middle_act)).astype(jnp.bfloat16)
    summit_sum = jax.ops.segment_sum(middle_out.astype(jnp.float32), owner_coarse, num_segments=TOP_NODES)
    summit_in = (summit_factor * summit_sum).astype(jnp.bfloat16)
    summit_act = jnp.dot(summit_in, summit_weight, preferred_element_type=jnp.float32)
    summit_out = jax.nn.silu(summit_act).astype(jnp.bfloat16)
    lifted = middle_out.astype(jnp.float32)[owner_fine] + summit_out.astype(jnp.float32)[owner_coarse[owner_fine]]
    mesh_out = (mesh_mid.astype(jnp.float32) + lifted).astype(jnp.bfloat16)
    decode_rows = mesh_out[decode_source]
    decode_pre = jnp.dot(decode_rows, decode_weight, preferred_element_type=jnp.float32) + decode_edges.astype(jnp.float32)
    grid_update = (grid_feats.astype(jnp.float32) + decode_factor * edge_sum(jax.nn.silu(decode_pre), decode_target, GRID)).astype(jnp.bfloat16)
    decode_live = (decode_target >= 0)[:, None]
    incoming = cotangent[jnp.maximum(decode_target, 0)].astype(jnp.float32) * decode_factor
    decode_slope = jnp.where(decode_live, incoming * silu_slope(decode_pre), 0.0).astype(jnp.bfloat16)
    decode_grad = jnp.dot(decode_rows.T, decode_slope, preferred_element_type=jnp.float32)
    passed = jnp.dot(decode_slope, decode_weight.T, preferred_element_type=jnp.float32)
    mesh_grad = jax.ops.segment_sum(passed, decode_source, num_segments=MESH)
    level_grad = jax.ops.segment_sum(mesh_grad, owner_fine, num_segments=MIDDLE)
    summit_total = jax.ops.segment_sum(level_grad, owner_coarse, num_segments=TOP_NODES)
    summit_slope = (summit_total * silu_slope(summit_act)).astype(jnp.bfloat16)
    summit_grad = jnp.dot(summit_in.T, summit_slope, preferred_element_type=jnp.float32)
    summit_back = jnp.dot(summit_slope, summit_weight.T, preferred_element_type=jnp.float32).astype(jnp.bfloat16)
    level_total = level_grad + summit_factor * summit_back.astype(jnp.float32)[owner_coarse]
    middle_slope = (level_total * silu_slope(middle_act)).astype(jnp.bfloat16)
    middle_grad = jnp.dot(middle_in.T, middle_slope, preferred_element_type=jnp.float32)
    middle_back = level_total + jnp.dot(middle_slope, middle_weight.T, preferred_element_type=jnp.float32)
    mesh_total = mesh_grad + middle_factor * middle_back[owner_fine]
    encode_live = (encode_target >= 0)[:, None]
    upstream = mesh_total[jnp.maximum(encode_target, 0)] * encode_factor
    encode_slope = jnp.where(encode_live, upstream * silu_slope(encode_pre), 0.0).astype(jnp.bfloat16)
    encode_grad = jnp.dot(encode_rows.T, encode_slope, preferred_element_type=jnp.float32)
    return grid_update, encode_grad, decode_grad, middle_grad, summit_grad
```

```python
import functools

import jax
import jax.numpy as jnp
from jax import lax
from jax.experimental import pallas as pl
from jax.experimental.pallas import tpu as pltpu
from jax.sharding import PartitionSpec as P

MESH = pl.DeviceIdType.MESH
TOP = 512
LANES = 128
LAYOUT = {64: (8, 2, 4), 4: (2, 1, 2)}
F32 = jnp.float32
BF16 = jnp.bfloat16


def nn(a, b):
    return lax.dot_general(a, b, (((1,), (0,)), ((), ())), preferred_element_type=F32)


def nt(a, b):
    return lax.dot_general(a, b, (((1,), (1,)), ((), ())), preferred_element_type=F32)


def tn(a, b):
    return lax.dot_general(a, b, (((0,), (0,)), ((), ())), preferred_element_type=F32)


def silu_pair(v):
    s = 0.5 * jnp.tanh(0.5 * v) + 0.5
    return v * s, s * (1.0 + v * (1.0 - s))


def ones_where(mask):
    return jnp.where(mask, 1.0, 0.0).astype(BF16)


def sum_halves(members, values):
    high = values.astype(BF16)
    low = (values - high.astype(F32)).astype(BF16)
    return nn(members, high) + nn(members, low)


def chunks(count, size, body):
    def step(i, carry):
        body(pl.ds(pl.multiple_of(i * size, size), size))
        return carry

    lax.fori_loop(0, count, step, 0)


class Spot:
    def __init__(self, tiles):
        self.nz, self.nyh, self.nx = LAYOUT[tiles]
        self.ny = 2 * self.nyh
        self.plane = self.ny * self.nx
        tile, sub = lax.axis_index("tile"), lax.axis_index("sub")
        self.tile, self.sub = tile, sub
        self.x = lax.rem(tile, self.nx)
        self.z = lax.div(tile, self.nx * self.nyh)
        yh = lax.rem(lax.div(tile, self.nx), self.nyh)
        self.core = lax.rem(sub, 2)
        self.y = yh * 2 + lax.div(sub, 2)
        self.p = self.y * self.nx + self.x
        self.device = tile * 4 + sub
        self.tiles = tiles

    def at(self, z, y, x, core):
        return (
            (z * self.nyh + lax.div(y, 2)) * self.nx + x,
            lax.rem(y, 2) * 2 + core,
        )

    def partner(self):
        return (self.tile, self.sub + 1 - 2 * self.core)

    def across(self):
        return (self.tile, lax.rem(self.sub + 2, 4))

    def beside(self, by):
        d = lax.rem(self.device + by + 4 * self.tiles, 4 * self.tiles)
        return (lax.div(d, 4), lax.rem(d, 4))

    def in_plane(self, k):
        y = lax.rem(self.y + k // self.nx, self.ny)
        x = lax.rem(self.x + k % self.nx, self.nx)
        return y * self.nx + x, self.at(self.z, y, x, self.core)

    def in_column(self, j):
        return self.at(lax.rem(self.z + j, self.nz), self.y, self.x, self.core)


def remote(src, dst, send, recv, where):
    return pltpu.make_async_remote_copy(
        src_ref=src,
        dst_ref=dst,
        send_sem=send,
        recv_sem=recv,
        device_id=where,
        device_id_type=MESH,
    )


class Total:
    def __init__(self, spot, slot, bufs):
        self.spot, self.slot = spot, slot
        own, pair, half, planes, column, full, self.ps, self.pr, self.qs, self.qr, self.zs, self.zr = bufs
        self.own, self.pair, self.half = own.at[slot], pair.at[slot], half.at[slot]
        self.planes, self.column, self.full = planes.at[slot], column.at[slot], full.at[slot]
        self.rows = TOP // 2
        self.block = self.rows // spot.plane

    def half_of(self, core):
        return pl.ds(pl.multiple_of(core * self.rows, self.rows), self.rows)

    def my_rows(self):
        s = self.spot
        start = s.core * self.rows + s.p * self.block
        return pl.ds(pl.multiple_of(start, self.block), self.block)

    def pair_copy(self, n):
        s = self.spot
        if n == 0:
            src, dst = self.own.at[self.half_of(1 - s.core)], self.pair
        else:
            src = dst = self.full.at[self.half_of(s.core)]
        return remote(src, dst, self.ps.at[self.slot, n], self.pr.at[self.slot, n], s.partner())

    def plane_copy(self, n, k):
        q, where = self.spot.in_plane(k)
        if n == 0:
            src = self.half.at[pl.ds(pl.multiple_of(q * self.block, self.block), self.block)]
            dst = self.planes.at[k]
        else:
            src = dst = self.full.at[self.my_rows()]
        return remote(src, dst, self.qs.at[self.slot, n, k], self.qr.at[self.slot, n, k], where)

    def column_copy(self, j):
        s = self.spot
        src = self.column.at[s.z]
        return remote(src, src, self.zs.at[self.slot, j], self.zr.at[self.slot, j], s.in_column(j))

    def step0(self):
        self.pair_copy(0).start()

    def step1(self):
        self.pair_copy(0).wait_recv()
        mine = self.own[self.half_of(self.spot.core), :].astype(F32)
        self.half[...] = (mine + self.pair[...].astype(F32)).astype(BF16)
        for k in range(1, self.spot.plane):
            self.plane_copy(0, k).start()

    def step2(self):
        s = self.spot
        start = pl.multiple_of(s.p * self.block, self.block)
        total = self.half[pl.ds(start, self.block), :].astype(F32)
        for k in range(1, s.plane):
            self.plane_copy(0, k).wait_recv()
        for k in range(1, s.plane):
            total = total + self.planes[k].astype(F32)
        self.column[s.z] = total.astype(BF16)
        for j in range(1, s.nz):
            self.column_copy(j).start()

    def step3(self, scale=None):
        s = self.spot
        for j in range(1, s.nz):
            self.column_copy(j).wait_recv()
        total = self.column[0].astype(F32)
        for j in range(1, s.nz):
            total = total + self.column[j].astype(F32)
        if scale is not None:
            total = total * scale
        self.full[self.my_rows(), :] = total.astype(BF16)
        for k in range(1, s.plane):
            self.plane_copy(1, k).start()

    def step4(self):
        for k in range(1, self.spot.plane):
            self.plane_copy(1, k).wait_recv()
        self.pair_copy(1).start()

    def step5(self):
        self.pair_copy(1).wait_recv()

    def drain(self):
        for n in range(2):
            self.pair_copy(n).wait_send()
            for k in range(1, self.spot.plane):
                self.plane_copy(n, k).wait_send()
        for j in range(1, self.spot.nz):
            self.column_copy(j).wait_send()


def kernel(
    tiles,
    grid_hbm,
    mesh_hbm,
    ee_hbm,
    de_hbm,
    esrc,
    etgt,
    dsrc,
    dtgt,
    fine,
    coarse,
    we_hbm,
    wd_hbm,
    wm_hbm,
    ws_hbm,
    cot_hbm,
    out_grid,
    out_e,
    out_d,
    out_m,
    out_s,
    gw,
    mesh,
    ee,
    de,
    cot,
    we,
    wd,
    wm,
    ws,
    ids,
    se,
    ste,
    me,
    mte,
    sd,
    std,
    md,
    mtd,
    fm,
    ft,
    kt,
    kc,
    cw,
    cwt,
    sile,
    ssle,
    sild,
    ssld,
    mid,
    sub_src,
    sub_dst,
    midin,
    midss,
    midout,
    base,
    sumss,
    sumout,
    mow,
    slope,
    tw,
    rw,
    rback,
    lev,
    meshg,
    up,
    sslope,
    sback,
    own,
    pair,
    half,
    planes,
    column,
    full,
    lsem,
    hs,
    hr,
    ss,
    sr,
    ps,
    pr,
    qs,
    qr,
    zs,
    zr,
):
    n = LANES
    d = mesh.shape[1]
    spot = Spot(tiles)
    n_enc, n_dec = ee.shape[0], de.shape[0]
    enc_factor, dec_factor = n / n_enc, n / n_dec
    mid_factor, top_factor = 0.25, TOP / (n * tiles)
    bufs = (own, pair, half, planes, column, full, ps, pr, qs, qr, zs, zr)
    t_sum, t_back, t_dec, t_mid, t_enc = (Total(spot, i, bufs) for i in range(5))

    loads = [
        pltpu.make_async_copy(src, dst, lsem.at[i])
        for i, (src, dst) in enumerate(
            (
                (grid_hbm, gw.at[pl.ds(n, n)]),
                (we_hbm, we),
                (ee_hbm, ee),
                (mesh_hbm, mesh),
                (wm_hbm, wm),
                (ws_hbm, ws),
                (wd_hbm, wd),
                (de_hbm, de),
                (cot_hbm, cot),
            )
        )
    ]
    for copy in loads:
        copy.start()

    barrier = pltpu.get_barrier_semaphore()
    greeted = [spot.beside(1), spot.beside(-1), spot.partner(), spot.across()]
    greeted += [spot.in_plane(k)[1] for k in range(1, spot.plane)]
    greeted += [spot.in_column(j) for j in range(1, spot.nz)]
    for where in greeted:
        pl.semaphore_signal(barrier, inc=1, device_id=where, device_id_type=MESH)

    lane = lax.broadcasted_iota(jnp.int32, (n, n), 1)
    row = lax.broadcasted_iota(jnp.int32, (n, n), 0)

    def spread(ref, i, shift):
        across = jnp.broadcast_to(ref[i : i + 1, :] - shift, (n, n))
        return across, jnp.transpose(across)

    def fill(ref, i, shift, wide, by_edge, by_node):
        across, down = spread(ref, i, shift)
        for j in range(wide):
            by_edge[i * n : (i + 1) * n, j * n : (j + 1) * n] = ones_where(down == lane + j * n)
            by_node[j * n : (j + 1) * n, i * n : (i + 1) * n] = ones_where(across == row + j * n)

    first = spot.device * n
    across, down = spread(fine, 0, spot.tile * n)
    fm[...] = ones_where(across == row)
    ft[...] = ones_where(down == lane)
    across_c, down_c = spread(coarse, 0, 0)
    coarse_of = jnp.sum(jnp.where(across == row, down_c, 0).astype(F32), axis=0, keepdims=True)
    ids[1] = jnp.broadcast_to(coarse_of, (8, n))
    for i in range(n_enc // n):
        fill(esrc, i, first - n, 3, se, ste)
        fill(etgt, i, first, 1, mte, me)

    def beside_copy(src, dst, i, by):
        return remote(src, dst, hs.at[i], hr.at[i], spot.beside(by))

    def both_ways(ref, i, low, mid_at, high):
        return (
            beside_copy(ref.at[mid_at], ref.at[low], i, 1),
            beside_copy(ref.at[mid_at], ref.at[high], i + 1, -1),
        )

    low, middle, high = (pl.ds(i * n, n) for i in range(3))
    loads[0].wait()
    pl.semaphore_wait(barrier, len(greeted))
    grid_halo = both_ways(gw, 0, low, middle, high)
    ids_halo = both_ways(ids, 2, 0, 1, 2)
    for copy in grid_halo + ids_halo:
        copy.start()

    for i in range(n_dec // n):
        fill(dsrc, i, first - n, 3, sd, std)
        fill(dtgt, i, first, 1, mtd, md)
    for j in range(TOP // n):
        kt[:, j * n : (j + 1) * n] = ones_where(down_c == lane + j * n)
        kc[j * n : (j + 1) * n, :] = ones_where(across_c == row + j * n)

    loads[1].wait()
    loads[2].wait()
    for copy in grid_halo:
        copy.wait_recv()

    def encode(at):
        rows = nn(se[at, :], gw[...]).astype(BF16)
        act, sloped = silu_pair(nn(rows, we[...]) + ee[at, :].astype(F32))
        sile[at, :] = act.astype(BF16)
        ssle[at, :] = sloped

    chunks(n_enc // 256, 256, encode)
    loads[3].wait()
    mid_value = (mesh[...].astype(F32) + enc_factor * nn(me[...], sile[...])).astype(BF16)
    mid[...] = mid_value

    def sub_copy(i):
        where = spot.partner() if i % 2 == 0 else spot.across()
        return remote(sub_src.at[i], sub_dst.at[i], ss.at[i], sr.at[i], where)

    sub_src[0] = nn(fm[...], mid_value).astype(BF16)
    sub_copy(0).start()
    sub_copy(0).wait_recv()
    sub_src[1] = (sub_src[0].astype(F32) + sub_dst[0].astype(F32)).astype(BF16)
    sub_copy(1).start()
    loads[4].wait()
    sub_copy(1).wait_recv()
    middle_in = (mid_factor * (sub_src[1].astype(F32) + sub_dst[1].astype(F32))).astype(BF16)
    midin[...] = middle_in
    act, sloped = silu_pair(nn(middle_in, wm[...]))
    midss[...] = sloped
    middle_out = (middle_in.astype(F32) + act).astype(BF16)
    wide_row = lax.broadcasted_iota(jnp.int32, (n, d), 0)
    mine = (wide_row >= spot.sub * (n // 4)) & (wide_row < (spot.sub + 1) * (n // 4))
    midout[...] = jnp.where(mine, middle_out.astype(F32), 0.0).astype(BF16)
    t_sum.own[...] = nn(kc[...], midout[...]).astype(BF16)
    t_sum.step0()
    base[middle, :] = mid[...].astype(F32) + nn(ft[...], middle_out)
    t_sum.step1()
    base_halo = both_ways(base, 4, low, middle, high)
    for copy in base_halo:
        copy.start()
    for copy in ids_halo:
        copy.wait_recv()
    for i in range(3):
        around = jnp.broadcast_to(ids[i, 0:1, :].astype(jnp.int32), (n, n))
        along = jnp.transpose(around)
        for j in range(TOP // n):
            cw[j * n : (j + 1) * n, i * n : (i + 1) * n] = ones_where(around == row + j * n)
            cwt[i * n : (i + 1) * n, j * n : (j + 1) * n] = ones_where(along == lane + j * n)
    t_sum.step2()
    t_sum.step3(top_factor)
    for i in range(5, 9):
        loads[i].wait()
    for copy in base_halo:
        copy.wait_recv()
    t_sum.step4()
    t_sum.step5()

    def top(at):
        act, sloped = silu_pair(nn(t_sum.full[at, :], ws[...]))
        sumout[at, :] = act.astype(BF16)
        sumss[at, :] = sloped

    chunks(TOP // 256, 256, top)

    def lift(at):
        mow[at, :] = (base[at, :] + nn(cwt[at, :], sumout[...])).astype(BF16)

    chunks(3, n, lift)

    def decode(at):
        rows = nn(sd[at, :], mow[...]).astype(BF16)
        act, sloped = silu_pair(nn(rows, wd[...]) + de[at, :].astype(F32))
        sild[at, :] = act.astype(BF16)
        incoming = nn(mtd[at, :], cot[...]) * dec_factor
        slope[at, :] = (incoming * sloped).astype(BF16)

    chunks(n_dec // 256, 256, decode)

    def back(at):
        spread_slope = nn(std[at, :], slope[pl.ds(0, n_dec), :]).astype(BF16)
        tw[at, :] = spread_slope
        rw[at, :] = nt(spread_slope, wd[...]).astype(BF16)

    chunks(3, n, back)

    def top_part(at):
        t_back.own[at, :] = nn(cw[at, :], rw[...]).astype(BF16)

    chunks(TOP // 256, 256, top_part)
    t_back.step0()
    back_halo = (
        beside_copy(rw.at[high], rback.at[0], 6, 1),
        beside_copy(rw.at[low], rback.at[1], 7, -1),
    )
    t_back.step1()
    for copy in back_halo:
        copy.start()
    t_dec.own[...] = tn(mow[...], tw[...]).astype(BF16)
    t_dec.step0()
    out_grid[...] = (
        gw[middle, :].astype(F32) + dec_factor * nn(md[...], sild[...])
    ).astype(BF16)
    for copy in back_halo:
        copy.wait_recv()
    mesh_grad = rw[middle, :].astype(F32) + rback[0].astype(F32) + rback[1].astype(F32)
    meshg[...] = mesh_grad
    sub_src[2] = sum_halves(fm[...], mesh_grad).astype(BF16)
    sub_copy(2).start()
    t_back.step2()
    t_dec.step1()
    sub_copy(2).wait_recv()
    sub_src[3] = (sub_src[2].astype(F32) + sub_dst[2].astype(F32)).astype(BF16)
    sub_copy(3).start()
    t_back.step3()
    t_dec.step2()
    sub_copy(3).wait_recv()
    lev[...] = sub_src[3].astype(F32) + sub_dst[3].astype(F32)
    t_back.step4()
    t_back.step5()

    def top_slope(at):
        value = (t_back.full[at, :].astype(F32) * sumss[at, :]).astype(BF16)
        sslope[at, :] = value
        sback[at, :] = nt(value, ws[...]).astype(BF16)

    chunks(TOP // 256, 256, top_slope)
    level_total = lev[...] + top_factor * nn(kt[...], sback[...])
    middle_slope = (level_total * midss[...]).astype(BF16)
    own_slope = jnp.where(mine, middle_slope.astype(F32), 0.0).astype(BF16)
    t_mid.own[...] = tn(midin[...], own_slope).astype(BF16)
    t_mid.step0()
    middle_back = level_total + nt(middle_slope, wm[...])
    mesh_total = meshg[...] + mid_factor * nn(ft[...], middle_back.astype(BF16))
    up[...] = mesh_total.astype(BF16)

    def encode_back(at):
        upstream = nn(mte[at, :], up[...]) * enc_factor
        slope[at, :] = (upstream * ssle[at, :]).astype(BF16)

    chunks(n_enc // 256, 256, encode_back)

    def encode_spread(at):
        tw[at, :] = nn(ste[at, :], slope[...]).astype(BF16)

    chunks(3, n, encode_spread)
    t_enc.own[...] = tn(gw[...], tw[...]).astype(BF16)
    t_enc.step0()
    t_mid.step1()
    t_enc.step1()
    t_dec.step3()
    t_mid.step2()
    t_enc.step2()
    out_s[...] = tn(t_sum.full[...], sslope[...]).astype(BF16)
    t_mid.step3()
    t_enc.step3()
    t_dec.step4()
    t_mid.step4()
    t_enc.step4()
    for total, out in ((t_dec, out_d), (t_mid, out_m), (t_enc, out_e)):
        total.step5()
        out[...] = total.full[...]
    for total in (t_sum, t_back, t_dec, t_mid, t_enc):
        total.drain()
    for copy in grid_halo + ids_halo + base_halo + back_halo:
        copy.wait_send()
    for i in range(4):
        sub_copy(i).wait_send()


def shards(tiles, *args):
    (gf, mf, ee, de, es, et, ds, dt, fine, coarse, we, wd, wm, ws, cot) = args
    n, d = mf.shape
    ne, nd = ee.shape[0], de.shape[0]
    nz, nyh, nx = LAYOUT[tiles]
    plane = 2 * nyh * nx
    hbm = pl.BlockSpec(memory_space=pl.ANY)
    vmem = pl.BlockSpec(memory_space=pltpu.VMEM)

    def v(*shape, dtype=BF16):
        return pltpu.VMEM(shape, dtype)

    sem = lambda *shape: pltpu.SemaphoreType.DMA(shape)
    wide = 3 * n
    scratch = [
        v(wide, d),
        v(n, d),
        v(ne, d),
        v(nd, d),
        v(n, d),
        v(d, d),
        v(d, d),
        v(d, d),
        v(d, d),
        v(3, 8, n, dtype=F32),
        v(ne, wide),
        v(wide, ne),
        v(n, ne),
        v(ne, n),
        v(nd, wide),
        v(wide, nd),
        v(n, nd),
        v(nd, n),
        v(n, n),
        v(n, n),
        v(n, TOP),
        v(TOP, n),
        v(TOP, wide),
        v(wide, TOP),
        v(ne, d),
        v(ne, d, dtype=F32),
        v(nd, d),
        v(nd, d, dtype=F32),
        v(n, d),
        v(4, n, d),
        v(4, n, d),
        v(n, d),
        v(n, d, dtype=F32),
        v(n, d),
        v(wide, d, dtype=F32),
        v(TOP, d, dtype=F32),
        v(TOP, d),
        v(wide, d),
        v(ne, d),
        v(wide, d),
        v(wide, d),
        v(2, n, d),
        v(n, d, dtype=F32),
        v(n, d, dtype=F32),
        v(n, d),
        v(TOP, d),
        v(TOP, d),
        v(5, TOP, d),
        v(5, TOP // 2, d),
        v(5, TOP // 2, d),
        v(5, plane, TOP // 2 // plane, d),
        v(5, nz, TOP // 2 // plane, d),
        v(5, TOP, d),
        sem(9),
        sem(8),
        sem(8),
        sem(4),
        sem(4),
        sem(5, 2),
        sem(5, 2),
        sem(5, 2, plane),
        sem(5, 2, plane),
        sem(5, nz),
        sem(5, nz),
    ]
    grid_update, eg, dg, mg, sg = pl.pallas_call(
        functools.partial(kernel, tiles),
        out_shape=[jax.ShapeDtypeStruct((n, d), BF16)]
        + [jax.ShapeDtypeStruct((d, d), BF16)] * 4,
        in_specs=[hbm] * 4 + [vmem] * 6 + [hbm] * 5,
        out_specs=[vmem] * 5,
        scratch_shapes=scratch,
        compiler_params=pltpu.CompilerParams(
            collective_id=0, has_side_effects=True, vmem_limit_bytes=60 * 1024 * 1024
        ),
    )(
        gf,
        mf,
        ee,
        de,
        *(i.reshape(-1, LANES) for i in (es, et, ds, dt, fine, coarse)),
        we,
        wd,
        wm,
        ws,
        cot,
    )
    return (grid_update, *(g.astype(F32) for g in (eg, dg, mg, sg)))


def solution(mesh):
    rows, ids = P(("tile", "sub"), None), P(("tile", "sub"))
    placed = (rows,) * 4 + (ids,) * 5 + (P("tile"),) + (P(),) * 4 + (rows,)
    return jax.shard_map(
        functools.partial(shards, mesh.shape["tile"]),
        mesh=mesh,
        in_specs=placed,
        out_specs=(rows, P(), P(), P(), P()),
        check_vma=False,
    )
```

```python
import functools

import jax
import jax.numpy as jnp
from jax import lax
from jax.experimental import pallas as pl
from jax.experimental.pallas import tpu as pltpu
from jax.sharding import PartitionSpec as P

MESH = pl.DeviceIdType.MESH
TOP = 512
LANES = 128
PARTS = 2
LAYOUT = {64: (8, 2, 4), 4: (2, 1, 2)}
F32 = jnp.float32
VMEM_BYTES = 67043328
BF16 = jnp.bfloat16


def nn(a, b):
    return lax.dot_general(a, b, (((1,), (0,)), ((), ())), preferred_element_type=F32)


def nt(a, b):
    return lax.dot_general(a, b, (((1,), (1,)), ((), ())), preferred_element_type=F32)


def tn(a, b):
    return lax.dot_general(a, b, (((0,), (0,)), ((), ())), preferred_element_type=F32)


def silu_pair(v):
    s = 0.5 * jnp.tanh(0.5 * v) + 0.5
    return v * s, s * (1.0 + v * (1.0 - s))


def ones_where(mask):
    return jnp.where(mask, 1.0, 0.0).astype(BF16)


def sum_halves(members, values):
    high = values.astype(BF16)
    low = (values - high.astype(F32)).astype(BF16)
    return nn(members, high) + nn(members, low)


def chunks(count, size, body):
    def step(i, carry):
        body(pl.ds(pl.multiple_of(i * size, size), size))
        return carry

    lax.fori_loop(0, count, step, 0)


class Spot:
    def __init__(self, tiles):
        self.nz, self.nyh, self.nx = LAYOUT[tiles]
        self.ny = 2 * self.nyh
        self.plane = self.ny * self.nx
        tile, sub = lax.axis_index("tile"), lax.axis_index("sub")
        self.tile, self.sub = tile, sub
        self.x = lax.rem(tile, self.nx)
        self.z = lax.div(tile, self.nx * self.nyh)
        yh = lax.rem(lax.div(tile, self.nx), self.nyh)
        self.core = lax.rem(sub, 2)
        self.y = yh * 2 + lax.div(sub, 2)
        self.p = self.y * self.nx + self.x
        self.device = tile * 4 + sub
        self.tiles = tiles

    def at(self, z, y, x, core):
        return (
            (z * self.nyh + lax.div(y, 2)) * self.nx + x,
            lax.rem(y, 2) * 2 + core,
        )

    def partner(self):
        return (self.tile, self.sub + 1 - 2 * self.core)

    def across(self):
        return (self.tile, lax.rem(self.sub + 2, 4))

    def diagonal(self):
        return (self.tile, 3 - self.sub)

    def beside(self, by):
        d = lax.rem(self.device + by + 4 * self.tiles, 4 * self.tiles)
        return (lax.div(d, 4), lax.rem(d, 4))

    def in_plane(self, k):
        y = lax.rem(self.y + k // self.nx, self.ny)
        x = lax.rem(self.x + k % self.nx, self.nx)
        return y * self.nx + x, self.at(self.z, y, x, self.core)

    def in_column(self, j):
        return self.at(lax.rem(self.z + j, self.nz), self.y, self.x, self.core)


def remote(src, dst, send, recv, where):
    return pltpu.make_async_remote_copy(
        src_ref=src,
        dst_ref=dst,
        send_sem=send,
        recv_sem=recv,
        device_id=where,
        device_id_type=MESH,
    )


def hops(k, n):
    return min(k, n - k)


class Total:
    def __init__(self, spot, slot, part, lead, bufs):
        self.spot = spot
        own, pair, half, planes, column, full, ps, pr, qs, qr, zs, zr = bufs
        width = own.shape[2] // PARTS
        i = slot * PARTS + part
        self.cols = pl.ds(part * width, width)
        self.own, self.full = own.at[slot], full.at[slot]
        self.pair, self.half, self.planes, self.column = pair.at[i], half.at[i], planes.at[i], column.at[i]
        self.ps, self.pr, self.qs, self.qr, self.zs, self.zr = (a.at[i] for a in (ps, pr, qs, qr, zs, zr))
        self.block = TOP // spot.plane
        self.leads, self.follows = spot.core == lead, spot.core != lead
        self.peers = sorted(
            range(1, spot.plane),
            key=lambda k: -hops(k // spot.nx, spot.ny) - hops(k % spot.nx, spot.nx),
        )
        self.rungs = sorted(range(1, spot.nz), key=lambda j: -hops(j, spot.nz))

    def rows_of(self, p):
        return pl.ds(pl.multiple_of(p * self.block, self.block), self.block)

    def pair_copy(self, n):
        if n == 0:
            src, dst = self.own.at[:, self.cols], self.pair
        else:
            src = dst = self.full.at[:, self.cols]
        return remote(src, dst, self.ps, self.pr, self.spot.partner())

    def plane_copy(self, n, k):
        q, where = self.spot.in_plane(k)
        if n == 0:
            src, dst = self.half.at[self.rows_of(q)], self.planes.at[k]
        else:
            src = dst = self.full.at[self.rows_of(self.spot.p), self.cols]
        return remote(src, dst, self.qs, self.qr.at[n], where)

    def column_copy(self, j):
        src = self.column.at[self.spot.z]
        return remote(src, src, self.zs, self.zr, self.spot.in_column(j))

    def plane_done(self, n):
        all_of = self.planes.at[pl.ds(1, self.spot.plane - 1)]
        return remote(all_of, all_of, self.qs, self.qr.at[n], self.spot.partner())

    def column_done(self):
        all_of = self.column.at[pl.ds(1, self.spot.nz - 1)]
        return remote(all_of, all_of, self.zs, self.zr, self.spot.partner())

    def step0(self):
        @pl.when(self.follows)
        def _():
            self.pair_copy(0).start()

    def step1(self):
        @pl.when(self.leads)
        def _():
            self.pair_copy(0).wait_recv()
            mine = self.own[:, self.cols].astype(F32)
            self.half[...] = (mine + self.pair[...].astype(F32)).astype(BF16)
            for k in self.peers:
                self.plane_copy(0, k).start()

    def step2(self):
        @pl.when(self.leads)
        def _():
            total = self.half[self.rows_of(self.spot.p), :].astype(F32)
            self.plane_done(0).wait_recv()
            for k in self.peers:
                total = total + self.planes[k].astype(F32)
            self.column[self.spot.z] = total.astype(BF16)
            for j in self.rungs:
                self.column_copy(j).start()

    def step3(self, scale=None):
        @pl.when(self.leads)
        def _():
            self.column_done().wait_recv()
            self.plane_done(0).wait_send()
            total = self.column[0].astype(F32)
            for j in range(1, self.spot.nz):
                total = total + self.column[j].astype(F32)
            if scale is not None:
                total = total * scale
            self.full[self.rows_of(self.spot.p), self.cols] = total.astype(BF16)
            for k in self.peers:
                self.plane_copy(1, k).start()

    def step4(self):
        @pl.when(self.leads)
        def _():
            self.plane_done(1).wait_recv()
            self.pair_copy(1).start()

    def step5(self):
        @pl.when(self.follows)
        def _():
            self.pair_copy(1).wait_recv()

    def drain(self):
        @pl.when(self.follows)
        def _():
            self.pair_copy(0).wait_send()

        @pl.when(self.leads)
        def _():
            self.pair_copy(1).wait_send()
            self.plane_done(1).wait_send()
            self.column_done().wait_send()


class Parts:
    def __init__(self, spot, slot, lead, bufs):
        self.own, self.full = bufs[0].at[slot], bufs[5].at[slot]
        self.parts = [Total(spot, slot, i, lead, bufs) for i in range(PARTS)]

    def fill(self, part_of):
        for part in self.parts:
            self.own[:, part.cols] = part_of(part.cols).astype(BF16)
            part.step0()

    def step(self, n, *given):
        for part in self.parts:
            getattr(part, f"step{n}")(*given)

    def drain(self):
        for part in self.parts:
            part.drain()


def kernel(
    tiles,
    grid_hbm,
    mesh_hbm,
    ee_hbm,
    de_hbm,
    esrc_hbm,
    etgt_hbm,
    dsrc_hbm,
    dtgt_hbm,
    fine_hbm,
    coarse_hbm,
    we_hbm,
    wd_hbm,
    wm_hbm,
    ws_hbm,
    cot_hbm,
    out_grid,
    out_e,
    out_d,
    out_m,
    out_s,
    esrc,
    etgt,
    dsrc,
    dtgt,
    fine,
    coarse,
    gw,
    mesh,
    ee,
    de,
    cot,
    we,
    wd,
    wm,
    ws,
    ids,
    se,
    ste,
    me,
    mte,
    sd,
    std,
    md,
    mtd,
    fm,
    ft,
    kt,
    kc,
    cw,
    cwt,
    sile,
    ssle,
    sild,
    mid,
    sub_src,
    sub_dst,
    midin,
    midss,
    midout,
    base,
    sumss,
    sumout,
    mow,
    slope,
    tw,
    rw,
    rback,
    lev,
    meshg,
    up,
    sslope,
    sback,
    ce,
    own_slope,
    gout,
    sgrad,
    own,
    pair,
    half,
    planes,
    column,
    full,
    lsem,
    osem,
    hs,
    hr,
    ss,
    sr,
    ps,
    pr,
    qs,
    qr,
    zs,
    zr,
):
    n = LANES
    d = mesh.shape[1]
    spot = Spot(tiles)
    n_enc, n_dec = ee.shape[0], de.shape[0]
    enc_factor, dec_factor = n / n_enc, n / n_dec
    mid_factor, top_factor = 0.25, TOP / (n * tiles)
    bufs = (own, pair, half, planes, column, full, ps, pr, qs, qr, zs, zr)
    t_sum, t_back, t_dec, t_mid, t_enc = (
        Parts(spot, i, lead, bufs) for i, lead in enumerate((1, 1, 0, 0, 1))
    )

    loads = [
        pltpu.make_async_copy(src, dst, lsem.at[i])
        for i, (src, dst) in enumerate(
            (
                (grid_hbm, gw.at[pl.ds(n, n)]),
                (we_hbm, we),
                (ee_hbm, ee),
                (mesh_hbm, mesh),
                (wm_hbm, wm),
                (ws_hbm, ws),
                (wd_hbm, wd),
                (de_hbm, de),
                (cot_hbm, cot),
                (fine_hbm, fine),
                (coarse_hbm, coarse),
                (esrc_hbm, esrc),
                (etgt_hbm, etgt),
                (dsrc_hbm, dsrc),
                (dtgt_hbm, dtgt),
            )
        )
    ]
    for copy in loads[9:] + loads[:9]:
        copy.start()

    barrier = pltpu.get_barrier_semaphore()
    greeted = [spot.beside(1), spot.beside(-1), spot.partner(), spot.across(), spot.diagonal()]
    greeted += [spot.in_plane(k)[1] for k in range(1, spot.plane)]
    greeted += [spot.in_column(j) for j in range(1, spot.nz)]
    for where in greeted:
        pl.semaphore_signal(barrier, inc=1, device_id=where, device_id_type=MESH)

    lane = lax.broadcasted_iota(jnp.int32, (n, n), 1)
    row = lax.broadcasted_iota(jnp.int32, (n, n), 0)

    def spread(ref, i, shift):
        across = jnp.broadcast_to(ref[i : i + 1, :] - shift, (n, n))
        return across, jnp.transpose(across)

    def fill(ref, i, shift, wide, by_edge, by_node):
        across, down = spread(ref, i, shift)
        for j in range(wide):
            by_edge[i * n : (i + 1) * n, j * n : (j + 1) * n] = ones_where(down == lane + j * n)
            by_node[j * n : (j + 1) * n, i * n : (i + 1) * n] = ones_where(across == row + j * n)

    for copy in loads[9:]:
        copy.wait()
    first = spot.device * n
    across, down = spread(fine, 0, spot.tile * n)
    fm[...] = ones_where(across == row)
    ft[...] = ones_where(down == lane)
    across_c, down_c = spread(coarse, 0, 0)
    coarse_of = jnp.sum(jnp.where(across == row, down_c, 0).astype(F32), axis=0, keepdims=True)
    ids[1] = jnp.broadcast_to(coarse_of, (8, n))
    for i in range(n_enc // n):
        fill(esrc, i, first - n, 3, se, ste)
        fill(etgt, i, first, 1, mte, me)

    def beside_copy(src, dst, i, by):
        return remote(src, dst, hs.at[i], hr.at[i], spot.beside(by))

    def both_ways(ref, i, low, mid_at, high):
        return (
            beside_copy(ref.at[mid_at], ref.at[low], i, 1),
            beside_copy(ref.at[mid_at], ref.at[high], i + 1, -1),
        )

    low, middle, high = (pl.ds(i * n, n) for i in range(3))
    loads[0].wait()
    pl.semaphore_wait(barrier, len(greeted))
    grid_halo = both_ways(gw, 0, low, middle, high)
    ids_halo = both_ways(ids, 2, 0, 1, 2)
    for copy in grid_halo + ids_halo:
        copy.start()

    for i in range(n_dec // n):
        fill(dsrc, i, first - n, 3, sd, std)
        fill(dtgt, i, first, 1, mtd, md)
    for j in range(TOP // n):
        kt[:, j * n : (j + 1) * n] = ones_where(down_c == lane + j * n)
        kc[j * n : (j + 1) * n, :] = ones_where(across_c == row + j * n)

    loads[1].wait()
    loads[2].wait()
    for copy in grid_halo:
        copy.wait_recv()

    def encode(at):
        rows = nn(se[at, :], gw[...]).astype(BF16)
        act, sloped = silu_pair(nn(rows, we[...]) + ee[at, :].astype(F32))
        sile[at, :] = act.astype(BF16)
        ssle[at, :] = sloped

    chunks(n_enc // 256, 256, encode)
    loads[3].wait()
    mid_value = (mesh[...].astype(F32) + enc_factor * nn(me[...], sile[...])).astype(BF16)
    mid[...] = mid_value

    def sub_copy(i):
        where = spot.partner() if i % 2 == 0 else spot.across()
        src, dst = sub_src.at[i], sub_dst.at[i]
        if i == 1:
            theirs = quarter(lax.rem(spot.sub + 2, 4))
            src, dst = src.at[theirs], dst.at[theirs]
        return remote(src, dst, ss.at[i], sr.at[i], where)

    def quarter(sub):
        return pl.ds(pl.multiple_of(sub * (n // 4), n // 4), n // 4)

    def quarter_copies():
        part = midin.at[quarter(spot.sub)]
        peers = (spot.partner(), spot.across(), spot.diagonal())
        return [remote(part, part, ss.at[4 + i], sr.at[4 + i], where) for i, where in enumerate(peers)]

    sub_src[0] = nn(fm[...], mid_value).astype(BF16)
    sub_copy(0).start()
    midout[...] = jnp.zeros_like(midout)
    sub_copy(0).wait_recv()
    sub_src[1] = (sub_src[0].astype(F32) + sub_dst[0].astype(F32)).astype(BF16)
    sub_copy(1).start()
    loads[4].wait()
    sub_copy(1).wait_recv()
    at = quarter(spot.sub)
    part_in = (mid_factor * (sub_src[1, at, :].astype(F32) + sub_dst[1, at, :].astype(F32))).astype(BF16)
    midin[at, :] = part_in
    midout[at, :] = (part_in.astype(F32) + silu_pair(nn(part_in, wm[...]))[0]).astype(BF16)
    t_sum.fill(lambda cols: nn(kc[...], midout[:, cols]))
    for copy in quarter_copies():
        copy.start()
    t_sum.step(1)
    for copy in ids_halo:
        copy.wait_recv()
    for i in range(3):
        around = jnp.broadcast_to(ids[i, 0:1, :].astype(jnp.int32), (n, n))
        along = jnp.transpose(around)
        for j in range(TOP // n):
            cw[j * n : (j + 1) * n, i * n : (i + 1) * n] = ones_where(around == row + j * n)
            cwt[i * n : (i + 1) * n, j * n : (j + 1) * n] = ones_where(along == lane + j * n)
    for copy in quarter_copies():
        copy.wait_recv()
    act, sloped = silu_pair(nn(midin[...], wm[...]))
    midss[...] = sloped
    middle_out = (midin[...].astype(F32) + act).astype(BF16)
    base[middle, :] = mid[...].astype(F32) + nn(ft[...], middle_out)
    base_halo = both_ways(base, 4, low, middle, high)

    def edge_tops(at):
        ce[at, :] = nn(cw[at, :], std[...]).astype(BF16)

    chunks(TOP // 256, 256, edge_tops)
    wide_row = lax.broadcasted_iota(jnp.int32, (n, d), 0)
    mine = (wide_row >= spot.sub * (n // 4)) & (wide_row < (spot.sub + 1) * (n // 4))
    t_sum.step(2)
    for copy in base_halo:
        copy.start()
    t_sum.step(3, top_factor)
    for i in range(5, 9):
        loads[i].wait()
    for copy in base_halo:
        copy.wait_recv()
    t_sum.step(4)
    t_sum.step(5)

    def top(at):
        act, sloped = silu_pair(nn(t_sum.full[at, :], ws[...]))
        sumout[at, :] = act.astype(BF16)
        sumss[at, :] = sloped

    chunks(TOP // 256, 256, top)

    def lift(at):
        mow[at, :] = (base[at, :] + nn(cwt[at, :], sumout[...])).astype(BF16)

    chunks(3, n, lift)

    def decode(at):
        rows = nn(sd[at, :], mow[...]).astype(BF16)
        act, sloped = silu_pair(nn(rows, wd[...]) + de[at, :].astype(F32))
        sild[at, :] = act.astype(BF16)
        incoming = nn(mtd[at, :], cot[...]) * dec_factor
        slope[at, :] = (incoming * sloped).astype(BF16)

    chunks(n_dec // 256, 256, decode)

    def top_edges(at):
        sslope[at, :] = nn(ce[at, :], slope[pl.ds(0, n_dec), :]).astype(BF16)

    chunks(TOP // 256, 256, top_edges)
    t_back.fill(lambda cols: nt(sslope[...], wd[cols, :]))
    t_back.step(1)
    def back(at):
        spread_slope = nn(std[at, :], slope[pl.ds(0, n_dec), :]).astype(BF16)
        tw[at, :] = spread_slope
        rw[at, :] = nt(spread_slope, wd[...]).astype(BF16)

    chunks(3, n, back)
    back_halo = (
        beside_copy(rw.at[high], rback.at[0], 6, 1),
        beside_copy(rw.at[low], rback.at[1], 7, -1),
    )
    for copy in back_halo:
        copy.start()
    t_dec.fill(lambda cols: tn(mow[...], tw[:, cols]))
    gout[...] = (gw[middle, :].astype(F32) + dec_factor * nn(md[...], sild[...])).astype(BF16)
    put = [
        pltpu.make_async_copy(src, dst, osem.at[i])
        for i, (src, dst) in enumerate(
            (
                (gout, out_grid),
                (sgrad, out_s),
                (t_dec.full, out_d),
                (t_mid.full, out_m),
                (t_enc.full, out_e),
            )
        )
    ]
    put[0].start()
    t_back.step(2)
    t_dec.step(1)
    for copy in back_halo:
        copy.wait_recv()
    mesh_grad = rw[middle, :].astype(F32) + rback[0].astype(F32) + rback[1].astype(F32)
    meshg[...] = mesh_grad
    sub_src[2] = sum_halves(fm[...], mesh_grad).astype(BF16)
    sub_copy(2).start()
    sub_copy(2).wait_recv()
    sub_src[3] = (sub_src[2].astype(F32) + sub_dst[2].astype(F32)).astype(BF16)
    sub_copy(3).start()
    t_back.step(3)
    t_dec.step(2)
    sub_copy(3).wait_recv()
    lev[...] = sub_src[3].astype(F32) + sub_dst[3].astype(F32)
    t_back.step(4)
    t_back.step(5)
    def top_slope(at):
        value = (t_back.full[at, :].astype(F32) * sumss[at, :]).astype(BF16)
        sslope[at, :] = value
        sback[at, :] = nt(value, ws[...]).astype(BF16)

    chunks(TOP // 256, 256, top_slope)
    level_total = lev[...] + top_factor * nn(kt[...], sback[...])
    middle_slope = (level_total * midss[...]).astype(BF16)
    own_slope[...] = jnp.where(mine, middle_slope.astype(F32), 0.0).astype(BF16)
    t_mid.fill(lambda cols: tn(midin[...], own_slope[:, cols]))
    middle_back = level_total + nt(middle_slope, wm[...])
    mesh_total = meshg[...] + mid_factor * nn(ft[...], middle_back.astype(BF16))
    up[...] = mesh_total.astype(BF16)
    t_dec.step(3)
    def encode_back(at):
        upstream = nn(mte[at, :], up[...]) * enc_factor
        slope[at, :] = (upstream * ssle[at, :]).astype(BF16)

    chunks(n_enc // 256, 256, encode_back)

    def encode_spread(at):
        tw[at, :] = nn(ste[at, :], slope[...]).astype(BF16)

    chunks(3, n, encode_spread)
    t_enc.fill(lambda cols: tn(gw[...], tw[:, cols]))
    t_mid.step(1)
    t_enc.step(1)
    sgrad[...] = tn(t_sum.full[...], sslope[...]).astype(BF16)
    put[1].start()
    t_dec.step(4)
    t_mid.step(2)
    t_enc.step(2)
    t_dec.step(5)
    put[2].start()
    t_mid.step(3)
    t_enc.step(3)
    t_mid.step(4)
    t_enc.step(4)
    t_mid.step(5)
    put[3].start()
    t_enc.step(5)
    put[4].start()
    for total in (t_sum, t_back, t_dec, t_mid, t_enc):
        total.drain()
    for copy in put:
        copy.wait()
    for copy in grid_halo + ids_halo + base_halo + back_halo:
        copy.wait_send()
    for copy in [sub_copy(i) for i in range(4)] + quarter_copies():
        copy.wait_send()


def widen(*refs):
    given, out = refs[:5], refs[5:10]
    rows, narrow, wide, in_sem, out_sem = refs[10:]
    sources = [rows] + [narrow.at[i] for i in range(4)]
    results = [rows] + [wide.at[i] for i in range(4)]
    taken = [pltpu.make_async_copy(a, b, in_sem.at[i]) for i, (a, b) in enumerate(zip(given, sources))]
    put = [pltpu.make_async_copy(a, b, out_sem.at[i]) for i, (a, b) in enumerate(zip(results, out))]
    for copy in taken:
        copy.start()
    for i in range(5):
        taken[i].wait()
        if i:
            results[i][...] = sources[i][...].astype(F32)
        put[i].start()
    for copy in put:
        copy.wait()


def shards(tiles, *args):
    (gf, mf, ee, de, es, et, ds, dt, fine, coarse, we, wd, wm, ws, cot) = args
    n, d = mf.shape
    ne, nd = ee.shape[0], de.shape[0]
    nz, nyh, nx = LAYOUT[tiles]
    plane = 2 * nyh * nx
    hbm = pl.BlockSpec(memory_space=pl.ANY)

    def v(*shape, dtype=BF16):
        return pltpu.VMEM(shape, dtype)

    sem = lambda *shape: pltpu.SemaphoreType.DMA(shape)
    wide, streams = 3 * n, 5 * PARTS
    scratch = [
        *(v(r // LANES, LANES, dtype=jnp.int32) for r in (ne, ne, nd, nd, n, n)),
        v(wide, d),
        v(n, d),
        v(ne, d),
        v(nd, d),
        v(n, d),
        v(d, d),
        v(d, d),
        v(d, d),
        v(d, d),
        v(3, 8, n, dtype=F32),
        v(ne, wide),
        v(wide, ne),
        v(n, ne),
        v(ne, n),
        v(nd, wide),
        v(wide, nd),
        v(n, nd),
        v(nd, n),
        v(n, n),
        v(n, n),
        v(n, TOP),
        v(TOP, n),
        v(TOP, wide),
        v(wide, TOP),
        v(ne, d),
        v(ne, d, dtype=F32),
        v(nd, d),
        v(n, d),
        v(4, n, d),
        v(4, n, d),
        v(n, d),
        v(n, d, dtype=F32),
        v(n, d),
        v(wide, d, dtype=F32),
        v(TOP, d, dtype=F32),
        v(TOP, d),
        v(wide, d),
        v(ne, d),
        v(wide, d),
        v(wide, d),
        v(2, n, d),
        v(n, d, dtype=F32),
        v(n, d, dtype=F32),
        v(n, d),
        v(TOP, d),
        v(TOP, d),
        v(TOP, nd),
        v(n, d),
        v(n, d),
        v(d, d),
        v(5, TOP, d),
        v(streams, TOP, d // PARTS),
        v(streams, TOP, d // PARTS),
        v(streams, plane, TOP // plane, d // PARTS),
        v(streams, nz, TOP // plane, d // PARTS),
        v(5, TOP, d),
        sem(15),
        sem(5),
        sem(8),
        sem(8),
        sem(7),
        sem(7),
        sem(streams),
        sem(streams),
        sem(streams),
        sem(streams, 2),
        sem(streams),
        sem(streams),
    ]
    results = pl.pallas_call(
        functools.partial(kernel, tiles),
        out_shape=[jax.ShapeDtypeStruct((n, d), BF16)]
        + [jax.ShapeDtypeStruct((d, d), BF16)] * 4,
        in_specs=[hbm] * 15,
        out_specs=[hbm] * 5,
        scratch_shapes=scratch,
        compiler_params=pltpu.CompilerParams(
            collective_id=0, has_side_effects=True, vmem_limit_bytes=VMEM_BYTES
        ),
    )(
        gf,
        mf,
        ee,
        de,
        *(i.reshape(-1, LANES) for i in (es, et, ds, dt, fine, coarse)),
        we,
        wd,
        wm,
        ws,
        cot,
    )
    return pl.pallas_call(
        widen,
        out_shape=[jax.ShapeDtypeStruct((n, d), BF16)]
        + [jax.ShapeDtypeStruct((d, d), F32)] * 4,
        in_specs=[hbm] * 5,
        out_specs=[hbm] * 5,
        scratch_shapes=[v(n, d), v(4, d, d), v(4, d, d, dtype=F32), sem(5), sem(5)],
        compiler_params=pltpu.CompilerParams(vmem_limit_bytes=VMEM_BYTES),
    )(*results)


def solution(mesh):
    rows, ids = P(("tile", "sub"), None), P(("tile", "sub"))
    placed = (rows,) * 4 + (ids,) * 5 + (P("tile"),) + (P(),) * 4 + (rows,)
    return jax.shard_map(
        functools.partial(shards, mesh.shape["tile"]),
        mesh=mesh,
        in_specs=placed,
        out_specs=(rows, P(), P(), P(), P()),
        check_vma=False,
    )
```
